32 devices in a mesh: group: 4 (over x, core), tensor: 8 (over z, y).
Axes of the slice: x: 2, y: 2, z: 4, core: 2. Of those that a mesh axis runs over, the one named last changes fastest.
Arguments:
- tokens: bfloat16 [128, 3, 8192], P(('group', 'tensor')), may hold values from -6 to 6
- norm_gain: float32 [8192], replicated, may hold values from 0.25 to 1.75
- w_qkv: bfloat16 [8192, 10240], P(None, 'tensor'), may hold values from -0.0625 to 0.0625
- w_out: bfloat16 [8192, 8192], P('tensor'), may hold values from -0.0625 to 0.0625
- lengths: int32 [32, 4], P(('group', 'tensor')), may hold values from 1 to 512, 1024 in all within a row
- migrate: int32 [32, 4], P(('group', 'tensor')), may hold values from 0 to 3, as said below
- page_order: int32 [32, 12], P(('group', 'tensor')), may hold values from 0 to 11, each once within a row
- kv_pool: bfloat16 [32, 12, 2, 8, 128, 128], P(('group', 'tensor')), as said below
Outputs:
- mixed: bfloat16 [128, 3, 8192], P(('group', 'tensor'))
The draws below stay inside these ranges and needn't reach their ends.
Inputs may be any that keep to these rules, and one draw needn't show every extreme that they name: `migrate`: on each device every group number is named by exactly 1 row. The 4 lengths of one device sum to 1024. `kv_pool`: cached keys and values of order one or more.
All inputs are finite; a program needn't handle non-finite values.
Results may differ from the reference program's by a relative error of at most 0.013.
Values may be sent and summed in bfloat16 or wider, within the bound.
No kernel may reach another device: no remote copies, remote signals or barrier semaphores. Data moves between devices by JAX's collectives and lax.ppermute only.
A program may use at most 128 MiB of HBM per device.

```python
import math
import jax
import jax.numpy as jnp
import numpy as np
from jax import lax

D = 8192
HEADS = 64
KV_HEADS = 8
HEAD_DIM = 128
PAGE = 128
MAX_PAGES = 4
STEPS = 3
ROW_DEV = 4
QKV = 10240
LEN_SUM = 1024
POOL = 12
DEVS = 32
ROWS_ALL = 128
N_GROUP = 4
N_TENSOR = 8


def draw_migrate(key, part):
    subkeys = jax.random.split(key, N_GROUP * N_TENSOR)

    def one_device(subkey):
        return jax.random.permutation(subkey, ROW_DEV)
    shuffled = jax.vmap(one_device)(subkeys)
    return (shuffled // (ROW_DEV // N_GROUP)).astype(jnp.int32)


def draw_kv_pool(key, part):
    shape = (N_GROUP * N_TENSOR, POOL, 2, KV_HEADS, PAGE, HEAD_DIM)
    return jax.random.normal(key, shape, jnp.float32).astype(jnp.bfloat16)


def block_levels(key, shape, pieces, smallest, high):
    level = 1.0
    for position, shards_of in pieces:
        steps = jax.random.uniform(jax.random.fold_in(jax.random.fold_in(key, 6), position), (shards_of,), jnp.float32, smallest / len(pieces), high / len(pieces))
        level = level * jnp.repeat(jnp.exp(steps), shape[position] // shards_of).reshape((-1,) + (1,) * (len(shape) - 1 - position))
    return level


def profile(number_of, total, reach, lean):
    portions = [(1 << 20) // math.isqrt(rank ** lean) + 1 for rank in range(2, number_of + 1)]
    surplus, given = total - reach - (number_of - 1), [1] * (number_of - 1)
    while surplus > 0:
        free = [i for i in range(number_of - 1) if given[i] < reach]
        pool, left = sum([portions[i] for i in free]), surplus
        for i in free:
            extra = min(reach - given[i], max(1, left * portions[i] // pool), surplus)
            given[i] = given[i] + extra
            surplus = surplus - extra
    return np.array([reach] + given)


def ragged_sizes(stream_key, count, total, most, lean):
    if count == 2:
        one = jax.random.randint(stream_key, (), max(1, total - most), min(most, total - 1) + 1)
        return jnp.stack([one, total - one])
    tallies = jnp.asarray(profile(count, total, most, lean), jnp.int32)
    couples = (count - 1) // 2
    donor, taker = tallies[1:1 + 2 * couples:2], tallies[2:2 + 2 * couples:2]
    room = jnp.minimum(donor - 1, most - taker)
    moved = jax.random.randint(jax.random.fold_in(stream_key, 1), (couples,), 0, 1 << 20) % (room + 1)
    tallies = tallies.at[1:1 + 2 * couples:2].set(donor - moved).at[2:2 + 2 * couples:2].set(taker + moved)
    return tallies[jax.random.permutation(jax.random.fold_in(stream_key, 2), count)]


def gaussian(key, shape, deviation, limit, cuts=(), kind=jnp.bfloat16):
    result = deviation * jax.random.normal(key, shape, jnp.float32)
    if cuts:
        result = result * block_levels(key, shape, cuts, -0.22, 0.18)
    return jnp.clip(result, -limit, limit).astype(kind)


def setup_inputs(seed: int = 0) -> dict:
    streams_of = jax.random.split(jax.random.key(seed), 9)
    tokens = gaussian(streams_of[0], (ROWS_ALL, STEPS, D), 1.0, 6.0, ((0, 32),))
    norm_gain = jnp.clip(1.0 + 0.15 * jax.random.normal(streams_of[1], (D,), jnp.float32), 0.25, 1.75)
    w_qkv = gaussian(streams_of[2], (D, QKV), D ** -0.5, 0.0625, ((1, 8),))
    w_out = gaussian(streams_of[3], (HEADS * HEAD_DIM, D), (HEADS * HEAD_DIM) ** -0.5, 0.0625, ((0, 8),))
    lengths = jax.vmap(lambda own: ragged_sizes(own, ROW_DEV, LEN_SUM, MAX_PAGES * PAGE, 2))(jax.random.split(streams_of[4], DEVS)).reshape((DEVS, ROW_DEV)).astype(jnp.int32)
    migrate = draw_migrate(jax.random.fold_in(streams_of[8], 71), 0)
    page_order = jax.vmap(lambda own: jax.random.permutation(own, POOL))(jax.random.split(streams_of[6], DEVS)).reshape((DEVS, POOL)).astype(jnp.int32)
    kv_pool = draw_kv_pool(jax.random.fold_in(streams_of[8], 71), 0)
    return {"tokens": tokens, "norm_gain": norm_gain, "w_qkv": w_qkv, "w_out": w_out, "lengths": lengths, "migrate": migrate, "page_order": page_order, "kv_pool": kv_pool}


EPS = 1e-05
ROPE_BASE = 500000.0
NEG_FILL = -1e+30

def rotate(values, positions):
    half_dim = values.shape[-1] // 2
    inverse = ROPE_BASE ** (-(jnp.arange(half_dim, dtype=jnp.float32) * 2.0 / values.shape[-1]))
    angles = positions.astype(jnp.float32)[..., None] * inverse
    cosine = jnp.cos(angles)[..., None, :]
    sine = jnp.sin(angles)[..., None, :]
    lower_half = values[..., :half_dim]
    upper_half = values[..., half_dim:]
    return jnp.concatenate([lower_half * cosine - upper_half * sine, upper_half * cosine + lower_half * sine], axis=-1)

def cache_stats(queries, pages, row_lens):
    row_total, steps_here, head_count, head_dim = queries.shape
    page_count = pages.shape[1]
    kv_heads = pages.shape[3]
    page_len = pages.shape[4]
    grouped = queries.reshape(row_total, steps_here, kv_heads, head_count // kv_heads, head_dim).astype(jnp.float32)
    scores = jnp.einsum('rskgd,rbktd->rskgbt', grouped, pages[:, :, 0].astype(jnp.float32)) * head_dim ** (-0.5)
    places = jnp.arange(page_count, dtype=jnp.int32)[:, None] * page_len + jnp.arange(page_len, dtype=jnp.int32)[None, :]
    inside = (places[None] < row_lens[:, None, None])[:, None, None, None]
    page_top = lax.optimization_barrier(jnp.max(jnp.where(inside, scores, NEG_FILL), axis=-1))
    weights = jnp.where(inside, jnp.exp(scores - page_top[..., None]), 0.0).astype(jnp.bfloat16)
    page_total = lax.optimization_barrier(jnp.sum(weights.astype(jnp.float32), axis=-1))
    page_acc = jnp.einsum('rskgbt,rbktd->rskgbd', weights.astype(jnp.float32), pages[:, :, 1].astype(jnp.float32))
    top_score = lax.optimization_barrier(jnp.max(page_top, axis=-1))
    page_scale = jnp.exp(page_top - top_score[..., None])
    return (top_score, lax.optimization_barrier(jnp.sum(page_scale * page_total, axis=-1)), lax.optimization_barrier(jnp.sum(page_scale[..., None] * page_acc, axis=-2)))

def finish(queries, cache_parts, all_keys, all_values, first_step):
    row_total, steps_here, head_count, head_dim = queries.shape
    kv_heads = all_keys.shape[2]
    grouped = queries.reshape(row_total, steps_here, kv_heads, head_count // kv_heads, head_dim).astype(jnp.float32)
    scores = jnp.einsum('rskgd,rukd->rskgu', grouped, all_keys.astype(jnp.float32)) * head_dim ** (-0.5)
    allowed = jnp.arange(all_keys.shape[1])[None, :] <= first_step + jnp.arange(steps_here)[:, None]
    allowed = allowed[None, :, None, None, :]
    new_top = lax.optimization_barrier(jnp.max(jnp.where(allowed, scores, NEG_FILL), axis=-1))
    weights = jnp.where(allowed, jnp.exp(scores - new_top[..., None]), 0.0).astype(jnp.bfloat16)
    new_total = lax.optimization_barrier(jnp.sum(weights.astype(jnp.float32), axis=-1))
    new_acc = jnp.einsum('rskgu,rukd->rskgd', weights.astype(jnp.float32), all_values.astype(jnp.float32))
    cache_top, cache_total, cache_acc = cache_parts
    top_score = jnp.maximum(cache_top, new_top)
    cache_scale = jnp.exp(cache_top - top_score)
    new_scale = jnp.exp(new_top - top_score)
    merged = (cache_scale[..., None] * cache_acc + new_scale[..., None] * new_acc) / (cache_scale * cache_total + new_scale * new_total)[..., None]
    return merged.reshape(row_total, steps_here, head_count * head_dim).astype(jnp.bfloat16)

def reference(tokens, norm_gain, w_qkv, w_out, lengths, migrate, page_order, kv_pool):
    devices = N_GROUP * N_TENSOR
    sendq = ROW_DEV // N_GROUP
    width_q = HEADS * HEAD_DIM
    width_k = KV_HEADS * HEAD_DIM
    slot_ids = jnp.arange(ROW_DEV, dtype=jnp.int32)
    order = jnp.argsort(migrate * ROW_DEV + slot_ids[None, :], axis=1).astype(jnp.int32)
    pages_used = (lengths + PAGE - 1) // PAGE
    offsets = (jnp.cumsum(pages_used, axis=1) - pages_used).astype(jnp.int32)
    group_ids = jnp.arange(N_GROUP, dtype=jnp.int32)[:, None, None]
    tensor_ids = jnp.arange(N_TENSOR, dtype=jnp.int32)[None, :, None]
    zero_block = jnp.zeros((N_GROUP, N_TENSOR, ROW_DEV), jnp.int32)
    old_device = ((slot_ids // sendq)[None, None, :] * N_TENSOR + tensor_ids + zero_block).reshape(devices, ROW_DEV)
    sorted_place = (group_ids * sendq + (slot_ids % sendq)[None, None, :] + zero_block).reshape(devices, ROW_DEV)
    old_slot = order[old_device, sorted_place]
    new_lengths = lengths[old_device, old_slot]
    first_page = offsets[old_device, old_slot]
    page_slots = jnp.clip(first_page[..., None] + jnp.arange(MAX_PAGES, dtype=jnp.int32), 0, POOL - 1).astype(jnp.int32)
    page_ids = page_order[old_device[..., None], page_slots]
    floats = tokens.astype(jnp.float32)
    normed = (floats * lax.rsqrt(lax.optimization_barrier(jnp.mean(floats * floats, axis=-1, keepdims=True)) + EPS) * norm_gain).astype(jnp.bfloat16)
    qkv = jnp.dot(normed.reshape(-1, D), w_qkv, preferred_element_type=jnp.float32).astype(jnp.bfloat16)
    qkv = qkv.reshape(ROWS_ALL, STEPS, QKV)
    positions = new_lengths.reshape(ROWS_ALL)[:, None] + jnp.arange(STEPS, dtype=jnp.int32)[None, :]
    queries = rotate(qkv[..., :width_q].reshape(ROWS_ALL, STEPS, HEADS, HEAD_DIM).astype(jnp.float32), positions).astype(jnp.bfloat16)
    new_keys = rotate(qkv[..., width_q:width_q + width_k].reshape(ROWS_ALL, STEPS, KV_HEADS, HEAD_DIM).astype(jnp.float32), positions).astype(jnp.bfloat16)
    new_values = qkv[..., width_q + width_k:].reshape(ROWS_ALL, STEPS, KV_HEADS, HEAD_DIM)

    def per_device(inputs):
        dev_queries, dev_keys, dev_values, dev_lens, dev_old, dev_pages = inputs
        pages = kv_pool[dev_old[:, None], dev_pages]
        parts = cache_stats(dev_queries, pages, dev_lens)
        return finish(dev_queries, parts, dev_keys, dev_values, 0)
    attended = lax.map(per_device, (queries.reshape(devices, ROW_DEV, STEPS, HEADS, HEAD_DIM), new_keys.reshape(devices, ROW_DEV, STEPS, KV_HEADS, HEAD_DIM), new_values.reshape(devices, ROW_DEV, STEPS, KV_HEADS, HEAD_DIM), new_lengths, old_device, page_ids))
    shard_cols = width_q // N_TENSOR
    attended = attended.reshape(ROWS_ALL * STEPS, N_TENSOR, shard_cols).transpose(1, 0, 2)
    weight_parts = w_out.reshape(N_TENSOR, shard_cols, D)

    def add_term(total, pair):
        term = jnp.dot(pair[0], pair[1], preferred_element_type=jnp.float32)
        return (total + lax.optimization_barrier(term.astype(jnp.bfloat16)).astype(jnp.float32), None)
    summed, unused = lax.scan(add_term, jnp.zeros((ROWS_ALL * STEPS, D), jnp.float32), (attended, weight_parts))
    return (floats + summed.reshape(ROWS_ALL, STEPS, D)).astype(jnp.bfloat16)
```

```python
import functools

import jax
import jax.numpy as jnp
from jax import lax
from jax.experimental import pallas as pl
from jax.experimental.pallas import tpu as pltpu
from jax.sharding import PartitionSpec as P

HEADS = 64
KV_HEADS = 8
HEAD_DIM = 128
PAGE = 128
MAX_PAGES = 4


EPS = 1e-05
ROPE_BASE = 500000.0
NEG_FILL = -1e30


def rotate(values, positions):
    half_dim = values.shape[-1] // 2
    inverse = ROPE_BASE ** (-(jnp.arange(half_dim, dtype=jnp.float32) * 2.0 / values.shape[-1]))
    angles = positions.astype(jnp.float32)[..., None] * inverse
    cosine = jnp.cos(angles)[..., None, :]
    sine = jnp.sin(angles)[..., None, :]
    lower_half = values[..., :half_dim]
    upper_half = values[..., half_dim:]
    return jnp.concatenate(
        [lower_half * cosine - upper_half * sine, upper_half * cosine + lower_half * sine], axis=-1
    )


def cache_stats(queries, pages, row_lens):
    row_total, steps_here, head_count, head_dim = queries.shape
    page_count = pages.shape[1]
    kv_heads = pages.shape[3]
    page_len = pages.shape[4]
    grouped = queries.reshape(row_total, steps_here, kv_heads, head_count // kv_heads, head_dim)
    scores = jnp.einsum(
        "rskgd,rbktd->rskgbt", grouped, pages[:, :, 0], preferred_element_type=jnp.float32
    ) * head_dim ** (-0.5)
    places = (
        jnp.arange(page_count, dtype=jnp.int32)[:, None] * page_len
        + jnp.arange(page_len, dtype=jnp.int32)[None, :]
    )
    inside = (places[None] < row_lens[:, None, None])[:, None, None, None]
    page_top = jnp.max(jnp.where(inside, scores, NEG_FILL), axis=-1)
    weights = jnp.where(inside, jnp.exp(scores - page_top[..., None]), 0.0).astype(jnp.bfloat16)
    page_total = jnp.sum(weights.astype(jnp.float32), axis=-1)
    page_acc = jnp.einsum(
        "rskgbt,rbktd->rskgbd", weights, pages[:, :, 1], preferred_element_type=jnp.float32
    )
    top_score = jnp.max(page_top, axis=-1)
    page_scale = jnp.exp(page_top - top_score[..., None])
    return (
        top_score,
        jnp.sum(page_scale * page_total, axis=-1),
        jnp.sum(page_scale[..., None] * page_acc, axis=-2),
    )


def finish(queries, cache_parts, all_keys, all_values):
    row_total, steps_here, head_count, head_dim = queries.shape
    kv_heads = all_keys.shape[2]
    grouped = queries.reshape(row_total, steps_here, kv_heads, head_count // kv_heads, head_dim)
    scores = jnp.einsum(
        "rskgd,rukd->rskgu", grouped, all_keys, preferred_element_type=jnp.float32
    ) * head_dim ** (-0.5)
    allowed = jnp.arange(all_keys.shape[1])[None, :] <= jnp.arange(steps_here)[:, None]
    allowed = allowed[None, :, None, None, :]
    new_top = jnp.max(jnp.where(allowed, scores, NEG_FILL), axis=-1)
    weights = jnp.where(allowed, jnp.exp(scores - new_top[..., None]), 0.0).astype(jnp.bfloat16)
    new_total = jnp.sum(weights.astype(jnp.float32), axis=-1)
    new_acc = jnp.einsum(
        "rskgu,rukd->rskgd", weights, all_values, preferred_element_type=jnp.float32
    )
    cache_top, cache_total, cache_acc = cache_parts
    top_score = jnp.maximum(cache_top, new_top)
    cache_scale = jnp.exp(cache_top - top_score)
    new_scale = jnp.exp(new_top - top_score)
    merged = (cache_scale[..., None] * cache_acc + new_scale[..., None] * new_acc) / (
        cache_scale * cache_total + new_scale * new_total
    )[..., None]
    return merged.reshape(row_total, steps_here, head_count * head_dim).astype(jnp.bfloat16)


def plain_device(tokens, norm_gain, w_qkv, w_out, lengths, migrate, page_order, kv_pool):
    row_lens = lengths[0]
    destinations = migrate[0]
    pool_order = page_order[0]
    page_pool = kv_pool[0]
    row_total = row_lens.shape[0]
    pool_size = page_pool.shape[0]
    slot_ids = jnp.arange(row_total, dtype=jnp.int32)
    sort_keys = destinations * row_total + slot_ids
    row_ranks = jnp.sum((sort_keys[None, :] < sort_keys[:, None]).astype(jnp.int32), axis=1)
    placing = row_ranks[:, None] == slot_ids[None, :]
    pages_used = (row_lens + PAGE - 1) // PAGE
    offsets = jnp.cumsum(pages_used) - pages_used
    sorted_lens = jnp.sum(jnp.where(placing, row_lens[:, None], 0), axis=0)
    sorted_first = jnp.sum(jnp.where(placing, offsets[:, None], 0), axis=0)
    page_slots = jnp.clip(
        sorted_first[:, None] + jnp.arange(MAX_PAGES, dtype=jnp.int32)[None, :], 0, pool_size - 1
    )
    home_pages = page_pool[pool_order[page_slots]]
    new_lens = lax.all_to_all(sorted_lens, "group", split_axis=0, concat_axis=0, tiled=True)
    moved_pages = lax.all_to_all(home_pages, "group", split_axis=0, concat_axis=0, tiled=True)
    width_q = HEADS * HEAD_DIM
    width_k = KV_HEADS * HEAD_DIM
    keys_so_far = jnp.zeros((row_total, 0, KV_HEADS, HEAD_DIM), jnp.bfloat16)
    values_so_far = jnp.zeros((row_total, 0, KV_HEADS, HEAD_DIM), jnp.bfloat16)
    steps_here = tokens.shape[1]
    floats = tokens.astype(jnp.float32)
    normed = (
        floats * lax.rsqrt(jnp.mean(floats * floats, axis=-1, keepdims=True) + EPS) * norm_gain
    ).astype(jnp.bfloat16)
    gathered = jnp.einsum(
        "rsd,dc->rsc",
        lax.all_gather(normed, "tensor", axis=0, tiled=True),
        w_qkv,
        preferred_element_type=jnp.float32,
    ).astype(jnp.bfloat16)
    full_rows = lax.all_to_all(gathered, "tensor", split_axis=0, concat_axis=2, tiled=True)
    positions = new_lens[:, None] + 0 + jnp.arange(steps_here, dtype=jnp.int32)[None, :]
    queries = rotate(
        full_rows[..., :width_q]
        .reshape(row_total, steps_here, HEADS, HEAD_DIM)
        .astype(jnp.float32),
        positions,
    ).astype(jnp.bfloat16)
    keys_here = rotate(
        full_rows[..., width_q : width_q + width_k]
        .reshape(row_total, steps_here, KV_HEADS, HEAD_DIM)
        .astype(jnp.float32),
        positions,
    ).astype(jnp.bfloat16)
    values_here = full_rows[..., width_q + width_k :].reshape(
        row_total, steps_here, KV_HEADS, HEAD_DIM
    )
    all_keys = jnp.concatenate([keys_so_far, keys_here], axis=1)
    all_values = jnp.concatenate([values_so_far, values_here], axis=1)
    attended = finish(queries, cache_stats(queries, moved_pages, new_lens), all_keys, all_values)
    spread = lax.all_to_all(attended, "tensor", split_axis=2, concat_axis=0, tiled=True)
    summed = lax.psum_scatter(
        jnp.einsum("rsc,cd->rsd", spread, w_out, preferred_element_type=jnp.float32).astype(
            jnp.bfloat16
        ),
        "tensor",
        scatter_dimension=0,
        tiled=True,
    ).astype(jnp.float32)
    output = (floats + summed).astype(jnp.bfloat16)
    return output


BOTH = ("tensor", "group")
IN_CHUNKS = 1
OUT_CHUNKS = 2


def project_kernel(order, *refs, peers, steps, slots, last, first):
    blocks = refs[:peers]
    weights = refs[peers]
    refs = refs[peers + 1 :]
    if not first:
        before, refs = refs[0], refs[1:]
    out, lhs, acc = refs[:3]
    step = pl.program_id(0)
    span = peers * slots
    for k in range(peers):
        for s in range(steps):
            start = s * span + k * slots
            lhs[start : start + slots, :] = blocks[k][s].astype(jnp.float32)
    part = jnp.dot(
        lhs[...].astype(jnp.bfloat16), weights[...], preferred_element_type=jnp.float32
    )

    @pl.when(step == 0)
    def _():
        acc[...] = part if first else before[...] + part

    @pl.when(step > 0)
    def _():
        acc[...] += part

    @pl.when(step == pl.num_programs(0) - 1)
    def _():
        if not last:
            out[...] = acc[...]
            return
        stage = refs[3]
        height = out.shape[1]
        lanes = out.shape[2]
        pieces = acc.shape[1] // lanes
        for c in range(pieces):
            for s in range(steps):
                stage[pl.ds(c * steps + s, span, stride=height), :] = acc[
                    s * span : (s + 1) * span, c * lanes : (c + 1) * lanes
                ]
        for extra in range(pieces * steps, height):
            stage[pl.ds(extra, span, stride=height), :] = jnp.zeros((span, lanes), jnp.float32)
        for k in range(peers):
            for i in range(slots):
                place = (k * slots + i) * height
                out[order[k] * slots + i] = stage[place : place + height, :].astype(jnp.bfloat16)


def project(order, blocks, weights, lo, hi, before, last):
    peers = len(blocks)
    steps, slots, _ = blocks[0].shape
    width = weights.shape[1]
    tile = 1024
    base = lo // tile
    rows = peers * steps * slots
    height = -(-(width // HEAD_DIM * steps) // 16) * 16
    first = before is None
    in_specs = [pl.BlockSpec((steps, slots, tile), lambda j, o: (0, 0, j))] * peers
    in_specs.append(pl.BlockSpec((tile, width), lambda j, o: (j + base, 0)))
    operands = list(blocks) + [weights]
    if not first:
        in_specs.append(pl.BlockSpec((rows, width), lambda j, o: (0, 0)))
        operands.append(before)
    scratch = [pltpu.VMEM((rows, tile), jnp.float32), pltpu.VMEM((rows, width), jnp.float32)]
    if last:
        shape = (peers * slots, height, HEAD_DIM)
        out_shape = jax.ShapeDtypeStruct(shape, jnp.bfloat16)
        out_spec = pl.BlockSpec(shape, lambda j, o: (0, 0, 0))
        scratch.append(pltpu.VMEM((peers * slots * height, HEAD_DIM), jnp.float32))
    else:
        out_shape = jax.ShapeDtypeStruct((rows, width), jnp.float32)
        out_spec = pl.BlockSpec((rows, width), lambda j, o: (0, 0))
    return pl.pallas_call(
        functools.partial(
            project_kernel, peers=peers, steps=steps, slots=slots, last=last, first=first
        ),
        grid_spec=pltpu.PrefetchScalarGridSpec(
            num_scalar_prefetch=1,
            grid=((hi - lo) // tile,),
            in_specs=in_specs,
            out_specs=out_spec,
            scratch_shapes=scratch,
        ),
        out_shape=out_shape,
        compiler_params=pltpu.CompilerParams(dimension_semantics=("arbitrary",)),
        cost_estimate=pl.CostEstimate(
            flops=2 * rows * width * (hi - lo),
            bytes_accessed=2 * width * (hi - lo),
            transcendentals=0,
        ),
        name="project",
    )(order, *operands)


def attend_kernel(
    lens, dest, order, qkv, cosine, sine, row_step, pool, out,
    pages, rows_f, fresh, queries, top, total, acc, sems, *, peers, steps,
):
    slots = cosine.shape[0]
    per_head = cosine.shape[1]
    kv_heads, page_len, dim = pages.shape[2:]
    per_peer = rows_f.shape[0] // peers
    scale = dim ** (-0.5)
    used = [(lens[0, j] + page_len - 1) // page_len for j in range(slots)]
    starts = [jnp.int32(0)]
    for j in range(slots - 1):
        starts.append(starts[-1] + used[j])

    def pick(values, i):
        found = jnp.int32(0)
        for j in range(slots):
            found = jnp.where(dest[0, j] == i, values[j], found)
        return found

    row_used = [pick(used, i) for i in range(slots)]
    row_start = [pick(starts, i) for i in range(slots)]
    row_len = [pick([lens[0, j] for j in range(slots)], i) for i in range(slots)]

    def fetch(slot, source):
        return pltpu.make_async_copy(pool.at[source], pages.at[slot], sems.at[slot])

    for i in range(slots):
        for b in range(MAX_PAGES):

            @pl.when(b < row_used[i])
            def _(i=i, b=b):
                fetch(i * MAX_PAGES + b, order[0, row_start[i] + b]).start()

    lane = lax.broadcasted_iota(jnp.int32, (per_head, page_len), 1)
    steps_of = row_step[...]
    fresh[...] = jnp.zeros(fresh.shape, fresh.dtype)

    def turn(values, i):
        return values * cosine[i] + pltpu.roll(values, dim // 2, 1) * sine[i]

    def block(h, keys, values, inside, first):
        rows = pl.ds(h * per_head, per_head)
        scores = (
            lax.dot_general(
                queries[h], keys, (((1,), (1,)), ((), ())), preferred_element_type=jnp.float32
            )
            * scale
        )
        scores = jnp.where(inside, scores, NEG_FILL)
        high = jnp.max(scores, axis=1, keepdims=True)
        if not first:
            old = top[rows, :]
            high = jnp.maximum(old, high)
        weights = jnp.where(inside, jnp.exp(scores - high), 0.0).astype(jnp.bfloat16)
        mass = jnp.sum(weights.astype(jnp.float32), axis=1, keepdims=True)
        part = jnp.dot(weights, values, preferred_element_type=jnp.float32)
        if first:
            top[rows, :] = jnp.broadcast_to(high, (per_head, dim))
            total[rows, :] = jnp.broadcast_to(mass, (per_head, dim))
            acc[rows, :] = part
        else:
            shrink = jnp.exp(old - high)
            top[rows, :] = high
            total[rows, :] = shrink * total[rows, :] + mass
            acc[rows, :] = shrink * acc[rows, :] + part

    for i in range(slots):
        for peer in range(peers):
            rows_f[peer * per_peer : (peer + 1) * per_peer, :] = qkv[
                peer * slots + i, 0:per_peer, :
            ].astype(jnp.float32)
        for h in range(kv_heads):
            queries[h] = turn(rows_f[h * per_head : (h + 1) * per_head, :], i).astype(jnp.bfloat16)
        edge = kv_heads * per_head
        span = kv_heads * steps
        fresh[0, 0:span, :] = turn(rows_f[edge : edge + span, :], i).astype(jnp.bfloat16)
        fresh[1, 0:span, :] = rows_f[edge + span : edge + 2 * span, :].astype(jnp.bfloat16)
        for h in range(kv_heads):
            inside = (lane >= h * steps) & (lane <= h * steps + steps_of)
            block(h, fresh[0], fresh[1], inside, True)

        def page(b, carry, i=i):
            slot = i * MAX_PAGES + b
            fetch(slot, 0).wait()
            inside = lane + b * page_len < row_len[i]
            for h in range(kv_heads):
                block(h, pages[slot, 0, h], pages[slot, 1, h], inside, False)
            return carry

        lax.fori_loop(0, row_used[i], page, 0)
        for h in range(kv_heads):
            rows = pl.ds(h * per_head, per_head)
            out[h * slots + i] = (acc[rows, :] / total[rows, :]).astype(jnp.bfloat16)


def attend(lengths, migrate, page_order, qkv, cosine, sine, row_step, pool, peers, steps):
    slots, per_head, dim = cosine.shape
    _, _, kv_heads, page_len, _ = pool.shape
    smem = pl.BlockSpec(memory_space=pltpu.SMEM)
    vmem = pl.BlockSpec(memory_space=pltpu.VMEM)
    per_peer = (kv_heads * per_head + 2 * kv_heads * steps) // peers
    scratch = [
        pltpu.VMEM((slots * MAX_PAGES,) + pool.shape[1:], pool.dtype),
        pltpu.VMEM((peers * per_peer, dim), jnp.float32),
        pltpu.VMEM((2, page_len, dim), jnp.bfloat16),
        pltpu.VMEM((kv_heads, per_head, dim), jnp.bfloat16),
        pltpu.VMEM((kv_heads * per_head, dim), jnp.float32),
        pltpu.VMEM((kv_heads * per_head, dim), jnp.float32),
        pltpu.VMEM((kv_heads * per_head, dim), jnp.float32),
        pltpu.SemaphoreType.DMA((slots * MAX_PAGES,)),
    ]
    work = slots * kv_heads * per_head * dim * page_len * MAX_PAGES
    return pl.pallas_call(
        functools.partial(attend_kernel, peers=peers, steps=steps),
        in_specs=[smem, smem, smem, vmem, vmem, vmem, vmem, pl.BlockSpec(memory_space=pl.ANY)],
        out_specs=vmem,
        out_shape=jax.ShapeDtypeStruct((kv_heads * slots, per_head, dim), jnp.bfloat16),
        scratch_shapes=scratch,
        cost_estimate=pl.CostEstimate(
            flops=4 * work, bytes_accessed=2 * pool.size, transcendentals=work // dim
        ),
        name="attend",
    )(lengths, migrate, page_order, qkv, cosine, sine, row_step, pool)


def output_kernel(order, attended, weights, *refs, peers, steps, slots):
    outs = refs[:peers]
    wide, lhs = refs[peers:]
    span = peers * slots
    height = attended.shape[1]
    lanes = attended.shape[2]

    @pl.when(pl.program_id(0) == 0)
    def _():
        for k in range(peers):
            for i in range(slots):
                place = (k * slots + i) * height
                wide[place : place + height, :] = attended[order[k] * slots + i].astype(jnp.float32)
        for c in range(height // steps):
            for s in range(steps):
                lhs[s * span : (s + 1) * span, c * lanes : (c + 1) * lanes] = wide[
                    pl.ds(c * steps + s, span, stride=height), :
                ].astype(jnp.bfloat16)

    term = jnp.dot(lhs[...], weights[...], preferred_element_type=jnp.float32)
    for k in range(peers):
        for s in range(steps):
            start = s * span + k * slots
            outs[k][s] = term[start : start + slots, :].astype(jnp.bfloat16)


def output_terms(order, attended, weights, lo, hi, slots, steps):
    span, height, lanes = attended.shape
    peers = span // slots
    depth = weights.shape[0]
    tile = 1024
    base = lo // tile
    shape = jax.ShapeDtypeStruct((steps, slots, hi - lo), jnp.bfloat16)
    return pl.pallas_call(
        functools.partial(output_kernel, peers=peers, steps=steps, slots=slots),
        grid_spec=pltpu.PrefetchScalarGridSpec(
            num_scalar_prefetch=1,
            grid=((hi - lo) // tile,),
            in_specs=[
                pl.BlockSpec(attended.shape, lambda j, o: (0, 0, 0)),
                pl.BlockSpec((depth, tile), lambda j, o: (0, j + base)),
            ],
            out_specs=[pl.BlockSpec((steps, slots, tile), lambda j, o: (0, 0, j))] * peers,
            scratch_shapes=[
                pltpu.VMEM((span * height, lanes), jnp.float32),
                pltpu.VMEM((span * steps, depth), jnp.bfloat16),
            ],
        ),
        out_shape=[shape] * peers,
        compiler_params=pltpu.CompilerParams(dimension_semantics=("arbitrary",)),
        cost_estimate=pl.CostEstimate(
            flops=2 * span * steps * depth * (hi - lo),
            bytes_accessed=2 * depth * (hi - lo),
            transcendentals=0,
        ),
        name="output_terms",
    )(order, attended, weights)


def swap(values, peers):
    return [values[0]] + [
        lax.ppermute(values[k], "tensor", [(t, t ^ k) for t in range(peers)])
        for k in range(1, peers)
    ]


def home_device(tokens, norm_gain, w_qkv, w_out, lengths, migrate, page_order, kv_pool, peers):
    slots, steps, width = tokens.shape
    own = lax.axis_index("tensor").astype(jnp.int32)
    order = jnp.bitwise_xor(own, jnp.arange(peers, dtype=jnp.int32))
    by_step = jnp.transpose(tokens, (1, 0, 2))
    floats = by_step.astype(jnp.float32)
    normed = (
        floats * lax.rsqrt(jnp.mean(floats * floats, axis=-1, keepdims=True) + EPS) * norm_gain
    ).astype(jnp.bfloat16)
    cut = width // IN_CHUNKS
    normed_parts = [normed[:, :, c * cut : (c + 1) * cut] for c in range(IN_CHUNKS)]
    gathered = [swap([part] * peers, peers) for part in normed_parts]
    projected = None
    for c in range(IN_CHUNKS):
        projected = project(
            order, gathered[c], w_qkv, c * cut, (c + 1) * cut, projected, c == IN_CHUNKS - 1
        )
    at_home = lax.all_to_all(projected, BOTH, split_axis=0, concat_axis=0, tiled=True)

    slot_ids = jnp.arange(slots, dtype=jnp.int32)
    sorted_lens = jnp.sum(
        jnp.where(migrate[0][:, None] == slot_ids[None, :], lengths[0][:, None], 0), axis=0
    )
    per_head = HEADS // KV_HEADS * steps
    row_step = jnp.arange(per_head, dtype=jnp.int32) % steps
    half = HEAD_DIM // 2
    lanes = jnp.arange(HEAD_DIM, dtype=jnp.int32)
    inverse = ROPE_BASE ** (-((lanes % half).astype(jnp.float32) * 2.0 / HEAD_DIM))
    positions = (sorted_lens[:, None] + row_step[None, :]).astype(jnp.float32)
    angles = positions[..., None] * inverse
    cosine = jnp.cos(angles)
    sine = jnp.where(lanes < half, -1.0, 1.0) * jnp.sin(angles)
    attended = attend(
        lengths,
        migrate,
        page_order,
        at_home,
        cosine,
        sine,
        jnp.broadcast_to(row_step[:, None], (per_head, HEAD_DIM)),
        kv_pool[0],
        peers,
        steps,
    )
    spread = lax.all_to_all(attended, BOTH, split_axis=0, concat_axis=0, tiled=True)
    cut = width // OUT_CHUNKS
    sums = []
    for c in range(OUT_CHUNKS):
        terms = output_terms(order, spread, w_out, c * cut, (c + 1) * cut, slots, steps)
        arrived = swap(list(terms), peers)
        whole = floats[:, :, c * cut : (c + 1) * cut]
        for term in arrived:
            whole = whole + term.astype(jnp.float32)
        sums.append(whole.astype(jnp.bfloat16))
    return jnp.transpose(jnp.concatenate(sums, axis=2), (1, 0, 2))


def per_device(tokens, norm_gain, w_qkv, w_out, lengths, migrate, page_order, kv_pool, peers, groups):
    arguments = (tokens, norm_gain, w_qkv, w_out, lengths, migrate, page_order, kv_pool)
    if peers == KV_HEADS and groups == tokens.shape[0] and w_qkv.shape[1] % HEAD_DIM == 0:
        return home_device(*arguments, peers)
    return plain_device(*arguments)


def solution(mesh):
    in_specs = (
        P(("group", "tensor"), None, None),
        P(),
        P(None, "tensor"),
        P("tensor", None),
        P(("group", "tensor"), None),
        P(("group", "tensor"), None),
        P(("group", "tensor"), None),
        P(("group", "tensor"), None, None, None, None, None),
    )
    out_specs = P(("group", "tensor"), None, None)
    body = functools.partial(per_device, peers=mesh.shape["tensor"], groups=mesh.shape["group"])
    return jax.shard_map(
        body, mesh=mesh, in_specs=in_specs, out_specs=out_specs, check_vma=False
    )
```

```python
import functools

import jax
import jax.numpy as jnp
from jax import lax
from jax.experimental import pallas as pl
from jax.experimental.pallas import tpu as pltpu
from jax.sharding import PartitionSpec as P

HEADS = 64
KV_HEADS = 8
HEAD_DIM = 128
PAGE = 128
MAX_PAGES = 4


EPS = 1e-05
ROPE_BASE = 500000.0
NEG_FILL = -1e30


def rotate(values, positions):
    half_dim = values.shape[-1] // 2
    inverse = ROPE_BASE ** (-(jnp.arange(half_dim, dtype=jnp.float32) * 2.0 / values.shape[-1]))
    angles = positions.astype(jnp.float32)[..., None] * inverse
    cosine = jnp.cos(angles)[..., None, :]
    sine = jnp.sin(angles)[..., None, :]
    lower_half = values[..., :half_dim]
    upper_half = values[..., half_dim:]
    return jnp.concatenate(
        [lower_half * cosine - upper_half * sine, upper_half * cosine + lower_half * sine], axis=-1
    )


def cache_stats(queries, pages, row_lens):
    row_total, steps_here, head_count, head_dim = queries.shape
    page_count = pages.shape[1]
    kv_heads = pages.shape[3]
    page_len = pages.shape[4]
    grouped = queries.reshape(row_total, steps_here, kv_heads, head_count // kv_heads, head_dim)
    scores = jnp.einsum(
        "rskgd,rbktd->rskgbt", grouped, pages[:, :, 0], preferred_element_type=jnp.float32
    ) * head_dim ** (-0.5)
    places = (
        jnp.arange(page_count, dtype=jnp.int32)[:, None] * page_len
        + jnp.arange(page_len, dtype=jnp.int32)[None, :]
    )
    inside = (places[None] < row_lens[:, None, None])[:, None, None, None]
    page_top = jnp.max(jnp.where(inside, scores, NEG_FILL), axis=-1)
    weights = jnp.where(inside, jnp.exp(scores - page_top[..., None]), 0.0).astype(jnp.bfloat16)
    page_total = jnp.sum(weights.astype(jnp.float32), axis=-1)
    page_acc = jnp.einsum(
        "rskgbt,rbktd->rskgbd", weights, pages[:, :, 1], preferred_element_type=jnp.float32
    )
    top_score = jnp.max(page_top, axis=-1)
    page_scale = jnp.exp(page_top - top_score[..., None])
    return (
        top_score,
        jnp.sum(page_scale * page_total, axis=-1),
        jnp.sum(page_scale[..., None] * page_acc, axis=-2),
    )


def finish(queries, cache_parts, all_keys, all_values):
    row_total, steps_here, head_count, head_dim = queries.shape
    kv_heads = all_keys.shape[2]
    grouped = queries.reshape(row_total, steps_here, kv_heads, head_count // kv_heads, head_dim)
    scores = jnp.einsum(
        "rskgd,rukd->rskgu", grouped, all_keys, preferred_element_type=jnp.float32
    ) * head_dim ** (-0.5)
    allowed = jnp.arange(all_keys.shape[1])[None, :] <= jnp.arange(steps_here)[:, None]
    allowed = allowed[None, :, None, None, :]
    new_top = jnp.max(jnp.where(allowed, scores, NEG_FILL), axis=-1)
    weights = jnp.where(allowed, jnp.exp(scores - new_top[..., None]), 0.0).astype(jnp.bfloat16)
    new_total = jnp.sum(weights.astype(jnp.float32), axis=-1)
    new_acc = jnp.einsum(
        "rskgu,rukd->rskgd", weights, all_values, preferred_element_type=jnp.float32
    )
    cache_top, cache_total, cache_acc = cache_parts
    top_score = jnp.maximum(cache_top, new_top)
    cache_scale = jnp.exp(cache_top - top_score)
    new_scale = jnp.exp(new_top - top_score)
    merged = (cache_scale[..., None] * cache_acc + new_scale[..., None] * new_acc) / (
        cache_scale * cache_total + new_scale * new_total
    )[..., None]
    return merged.reshape(row_total, steps_here, head_count * head_dim).astype(jnp.bfloat16)


def plain_device(tokens, norm_gain, w_qkv, w_out, lengths, migrate, page_order, kv_pool):
    row_lens = lengths[0]
    destinations = migrate[0]
    pool_order = page_order[0]
    page_pool = kv_pool[0]
    row_total = row_lens.shape[0]
    pool_size = page_pool.shape[0]
    slot_ids = jnp.arange(row_total, dtype=jnp.int32)
    sort_keys = destinations * row_total + slot_ids
    row_ranks = jnp.sum((sort_keys[None, :] < sort_keys[:, None]).astype(jnp.int32), axis=1)
    placing = row_ranks[:, None] == slot_ids[None, :]
    pages_used = (row_lens + PAGE - 1) // PAGE
    offsets = jnp.cumsum(pages_used) - pages_used
    sorted_lens = jnp.sum(jnp.where(placing, row_lens[:, None], 0), axis=0)
    sorted_first = jnp.sum(jnp.where(placing, offsets[:, None], 0), axis=0)
    page_slots = jnp.clip(
        sorted_first[:, None] + jnp.arange(MAX_PAGES, dtype=jnp.int32)[None, :], 0, pool_size - 1
    )
    home_pages = page_pool[pool_order[page_slots]]
    new_lens = lax.all_to_all(sorted_lens, "group", split_axis=0, concat_axis=0, tiled=True)
    moved_pages = lax.all_to_all(home_pages, "group", split_axis=0, concat_axis=0, tiled=True)
    width_q = HEADS * HEAD_DIM
    width_k = KV_HEADS * HEAD_DIM
    keys_so_far = jnp.zeros((row_total, 0, KV_HEADS, HEAD_DIM), jnp.bfloat16)
    values_so_far = jnp.zeros((row_total, 0, KV_HEADS, HEAD_DIM), jnp.bfloat16)
    steps_here = tokens.shape[1]
    floats = tokens.astype(jnp.float32)
    normed = (
        floats * lax.rsqrt(jnp.mean(floats * floats, axis=-1, keepdims=True) + EPS) * norm_gain
    ).astype(jnp.bfloat16)
    gathered = jnp.einsum(
        "rsd,dc->rsc",
        lax.all_gather(normed, "tensor", axis=0, tiled=True),
        w_qkv,
        preferred_element_type=jnp.float32,
    ).astype(jnp.bfloat16)
    full_rows = lax.all_to_all(gathered, "tensor", split_axis=0, concat_axis=2, tiled=True)
    positions = new_lens[:, None] + 0 + jnp.arange(steps_here, dtype=jnp.int32)[None, :]
    queries = rotate(
        full_rows[..., :width_q]
        .reshape(row_total, steps_here, HEADS, HEAD_DIM)
        .astype(jnp.float32),
        positions,
    ).astype(jnp.bfloat16)
    keys_here = rotate(
        full_rows[..., width_q : width_q + width_k]
        .reshape(row_total, steps_here, KV_HEADS, HEAD_DIM)
        .astype(jnp.float32),
        positions,
    ).astype(jnp.bfloat16)
    values_here = full_rows[..., width_q + width_k :].reshape(
        row_total, steps_here, KV_HEADS, HEAD_DIM
    )
    all_keys = jnp.concatenate([keys_so_far, keys_here], axis=1)
    all_values = jnp.concatenate([values_so_far, values_here], axis=1)
    attended = finish(queries, cache_stats(queries, moved_pages, new_lens), all_keys, all_values)
    spread = lax.all_to_all(attended, "tensor", split_axis=2, concat_axis=0, tiled=True)
    summed = lax.psum_scatter(
        jnp.einsum("rsc,cd->rsd", spread, w_out, preferred_element_type=jnp.float32).astype(
            jnp.bfloat16
        ),
        "tensor",
        scatter_dimension=0,
        tiled=True,
    ).astype(jnp.float32)
    output = (floats + summed).astype(jnp.bfloat16)
    return output


BOTH = ("tensor", "group")
IN_CUTS = (0, 4096, 8192)
OUT_CUTS = (0, 4096, 8192)
DIRECT_IN = False


def project_kernel(order, *refs, places, tile, lo, last, first):
    blocks = refs[: len(places)]
    weights = refs[len(places)]
    refs = refs[len(places) + 1 :]
    if not first:
        before, refs = refs[0], refs[1:]
    out, lhs, tiles, acc = refs[:4]
    sems = refs[-1]
    peers = order.shape[0]
    _, steps, slots, depth = blocks[0].shape
    span = peers * slots
    count = depth // tile

    def fetch(j):
        return pltpu.make_async_copy(
            weights.at[pl.ds(pl.multiple_of(lo + j * tile, tile), tile), :], tiles.at[j], sems.at[j]
        )

    for j in range(count):
        fetch(j).start()
    for block, ks in zip(blocks, places):
        for n, k in enumerate(ks):
            for s in range(steps):
                start = s * span + k * slots
                for j in range(count):
                    lhs[j, start : start + slots, :] = block[
                        n, s, :, j * tile : (j + 1) * tile
                    ].astype(jnp.float32)
    if not first:
        acc[...] = before[...]

    def part(j):
        fetch(j).wait()
        return jnp.dot(
            lhs[j].astype(jnp.bfloat16), tiles[j], preferred_element_type=jnp.float32
        )

    if first:
        acc[...] = part(0)

    def step(j, carry):
        acc[...] += part(j)
        return carry

    lax.fori_loop(1 if first else 0, count, step, 0)
    if not last:
        out[...] = acc[...]
        return
    stage = refs[4]
    height = out.shape[1]
    lanes = out.shape[2]
    pieces = acc.shape[1] // lanes
    for c in range(pieces):
        for s in range(steps):
            stage[pl.ds(c * steps + s, span, stride=height), :] = acc[
                s * span : (s + 1) * span, c * lanes : (c + 1) * lanes
            ]
    for extra in range(pieces * steps, height):
        stage[pl.ds(extra, span, stride=height), :] = jnp.zeros((span, lanes), jnp.float32)
    for k in range(peers):
        for i in range(slots):
            place = (k * slots + i) * height
            out[order[k] * slots + i] = stage[place : place + height, :].astype(jnp.bfloat16)


def project(order, blocks, places, weights, lo, hi, before, last):
    peers = order.shape[0]
    _, steps, slots, depth = blocks[0].shape
    width = weights.shape[1]
    tile = 512
    rows = peers * steps * slots
    height = -(-(width // HEAD_DIM * steps) // 16) * 16
    first = before is None
    vmem = pl.BlockSpec(memory_space=pltpu.VMEM)
    in_specs = [pl.BlockSpec(memory_space=pltpu.SMEM)] + [vmem] * len(blocks)
    in_specs.append(pl.BlockSpec(memory_space=pl.ANY))
    operands = list(blocks) + [weights]
    if not first:
        in_specs.append(vmem)
        operands.append(before)
    scratch = [
        pltpu.VMEM((depth // tile, rows, tile), jnp.float32),
        pltpu.VMEM((depth // tile, tile, width), jnp.bfloat16),
        pltpu.VMEM((rows, width), jnp.float32),
    ]
    if last:
        out_shape = jax.ShapeDtypeStruct((peers * slots, height, HEAD_DIM), jnp.bfloat16)
        scratch.append(pltpu.VMEM((peers * slots * height, HEAD_DIM), jnp.float32))
    else:
        out_shape = jax.ShapeDtypeStruct((rows, width), jnp.float32)
    scratch.append(pltpu.SemaphoreType.DMA((depth // tile,)))
    return pl.pallas_call(
        functools.partial(
            project_kernel, places=places, tile=tile, lo=lo, last=last, first=first
        ),
        in_specs=in_specs,
        out_specs=vmem,
        scratch_shapes=scratch,
        out_shape=out_shape,
        cost_estimate=pl.CostEstimate(
            flops=2 * rows * width * (hi - lo),
            bytes_accessed=2 * width * (hi - lo),
            transcendentals=0,
        ),
        name="project",
    )(order, *operands)


def attend_kernel(
    lens, dest, order, qkv, cosine, sine, row_step, pool, out,
    pages, rows_f, fresh, queries, sems, *, peers, steps,
):
    slots = cosine.shape[0]
    per_head = cosine.shape[1]
    kv_heads, page_len, dim = pages.shape[2:]
    per_peer = rows_f.shape[1] // peers
    scale = dim ** (-0.5)
    used = [(lens[0, j] + page_len - 1) // page_len for j in range(slots)]
    starts = [jnp.int32(0)]
    for j in range(slots - 1):
        starts.append(starts[-1] + used[j])

    def pick(values, i):
        found = jnp.int32(0)
        for j in range(slots):
            found = jnp.where(dest[0, j] == i, values[j], found)
        return found

    row_used = [pick(used, i) for i in range(slots)]
    row_start = [pick(starts, i) for i in range(slots)]
    row_len = [pick([lens[0, j] for j in range(slots)], i) for i in range(slots)]

    def fetch(slot, source):
        return pltpu.make_async_copy(pool.at[source], pages.at[slot], sems.at[slot])

    for i in range(slots):
        for b in range(MAX_PAGES):

            @pl.when(b < row_used[i])
            def _(i=i, b=b):
                fetch(i * MAX_PAGES + b, order[0, row_start[i] + b]).start()

    lane = lax.broadcasted_iota(jnp.int32, (per_head, page_len), 1)
    steps_of = row_step[...]
    edge = kv_heads * per_head
    span = kv_heads * steps
    fresh[...] = jnp.zeros(fresh.shape, fresh.dtype)

    def turn(values, i):
        return values * cosine[i] + pltpu.roll(values, dim // 2, 1) * sine[i]

    for i in range(slots):
        for peer in range(peers):
            rows_f[i, peer * per_peer : (peer + 1) * per_peer, :] = qkv[
                peer * slots + i, 0:per_peer, :
            ].astype(jnp.float32)
        for h in range(kv_heads):
            queries[i, h] = turn(
                rows_f[i, h * per_head : (h + 1) * per_head, :], i
            ).astype(jnp.bfloat16)
        fresh[i, 0, 0:span, :] = turn(rows_f[i, edge : edge + span, :], i).astype(jnp.bfloat16)
        fresh[i, 1, 0:span, :] = rows_f[i, edge + span : edge + 2 * span, :].astype(jnp.bfloat16)

    for i in range(slots):
        for b in range(MAX_PAGES):
            slot = i * MAX_PAGES + b

            @pl.when(b < row_used[i])
            def _(slot=slot):
                fetch(slot, 0).wait()

            @pl.when(b >= row_used[i])
            def _(slot=slot):
                pages[slot, 1] = jnp.zeros(pages.shape[2:], pages.dtype)

    together = 4
    for i in range(slots):
        live = [lane + b * page_len < row_len[i] for b in range(MAX_PAGES)]
        for base in range(0, kv_heads, together):
            group = range(base, base + together)

            def score(h, keys, inside):
                found = lax.dot_general(
                    queries[i, h], keys, (((1,), (1,)), ((), ())),
                    preferred_element_type=jnp.float32,
                )
                return jnp.where(inside, found * scale, NEG_FILL)

            scores = [
                [
                    score(h, pages[i * MAX_PAGES + b, 0, h], live[b])
                    for b in range(MAX_PAGES)
                ]
                + [
                    score(
                        h,
                        fresh[i, 0],
                        (lane >= h * steps) & (lane <= h * steps + steps_of),
                    )
                ]
                for h in group
            ]
            tops = [
                jnp.max(functools.reduce(jnp.maximum, row), axis=1, keepdims=True) for row in scores
            ]
            weights = [
                [jnp.exp(block - high).astype(jnp.bfloat16) for block in row]
                for row, high in zip(scores, tops)
            ]
            sums = [
                jnp.sum(
                    functools.reduce(jnp.add, [w.astype(jnp.float32) for w in row]),
                    axis=1,
                    keepdims=True,
                )
                for row in weights
            ]
            for h, row, mass in zip(group, weights, sums):
                total = jnp.dot(row[-1], fresh[i, 1], preferred_element_type=jnp.float32)
                for b in range(MAX_PAGES):
                    total += jnp.dot(
                        row[b],
                        pages[i * MAX_PAGES + b, 1, h],
                        preferred_element_type=jnp.float32,
                    )
                out[h * slots + i] = (total / mass).astype(jnp.bfloat16)


def attend(lengths, migrate, page_order, qkv, cosine, sine, row_step, pool, peers, steps):
    slots, per_head, dim = cosine.shape
    _, _, kv_heads, page_len, _ = pool.shape
    smem = pl.BlockSpec(memory_space=pltpu.SMEM)
    vmem = pl.BlockSpec(memory_space=pltpu.VMEM)
    per_peer = (kv_heads * per_head + 2 * kv_heads * steps) // peers
    scratch = [
        pltpu.VMEM((slots * MAX_PAGES,) + pool.shape[1:], pool.dtype),
        pltpu.VMEM((slots, peers * per_peer, dim), jnp.float32),
        pltpu.VMEM((slots, 2, page_len, dim), jnp.bfloat16),
        pltpu.VMEM((slots, kv_heads, per_head, dim), jnp.bfloat16),
        pltpu.SemaphoreType.DMA((slots * MAX_PAGES,)),
    ]
    work = slots * kv_heads * per_head * dim * page_len * MAX_PAGES
    return pl.pallas_call(
        functools.partial(attend_kernel, peers=peers, steps=steps),
        in_specs=[smem, smem, smem, vmem, vmem, vmem, vmem, pl.BlockSpec(memory_space=pl.ANY)],
        out_specs=vmem,
        out_shape=jax.ShapeDtypeStruct((kv_heads * slots, per_head, dim), jnp.bfloat16),
        scratch_shapes=scratch,
        cost_estimate=pl.CostEstimate(
            flops=4 * work, bytes_accessed=2 * pool.size, transcendentals=work // dim
        ),
        name="attend",
    )(lengths, migrate, page_order, qkv, cosine, sine, row_step, pool)


def output_kernel(order, attended, weights, near, far, wide, lhs, tiles, sems, *, steps, lo):
    peers = order.shape[0]
    span, height, lanes = attended.shape
    slots = span // peers
    count, _, tile = tiles.shape

    def fetch(j):
        return pltpu.make_async_copy(
            weights.at[:, pl.ds(lo + j * tile, tile)], tiles.at[j], sems.at[j]
        )

    for j in range(count):
        fetch(j).start()
    for k in range(peers):
        for i in range(slots):
            place = (k * slots + i) * height
            wide[place : place + height, :] = attended[order[k] * slots + i].astype(jnp.float32)
    for c in range(height // steps):
        for s in range(steps):
            lhs[s * span : (s + 1) * span, c * lanes : (c + 1) * lanes] = wide[
                pl.ds(c * steps + s, span, stride=height), :
            ].astype(jnp.bfloat16)
    for j in range(count):
        fetch(j).wait()
        term = jnp.dot(lhs[...], tiles[j], preferred_element_type=jnp.float32)
        for k in range(peers):
            for s in range(steps):
                start = s * span + k * slots
                outs = far if k % 2 else near
                outs[k // 2, s, :, j * tile : (j + 1) * tile] = term[
                    start : start + slots, :
                ].astype(jnp.bfloat16)


def output_terms(order, attended, weights, lo, hi, slots, steps):
    span, height, lanes = attended.shape
    depth = weights.shape[0]
    tile = 512
    shape = jax.ShapeDtypeStruct((span // slots // 2, steps, slots, hi - lo), jnp.bfloat16)
    vmem = pl.BlockSpec(memory_space=pltpu.VMEM)
    return pl.pallas_call(
        functools.partial(output_kernel, steps=steps, lo=lo),
        in_specs=[
            pl.BlockSpec(memory_space=pltpu.SMEM), vmem, pl.BlockSpec(memory_space=pl.ANY)
        ],
        out_specs=[vmem, vmem],
        scratch_shapes=[
            pltpu.VMEM((span * height, lanes), jnp.float32),
            pltpu.VMEM((span * steps, depth), jnp.bfloat16),
            pltpu.VMEM(((hi - lo) // tile, depth, tile), jnp.bfloat16),
            pltpu.SemaphoreType.DMA(((hi - lo) // tile,)),
        ],
        out_shape=[shape, shape],
        cost_estimate=pl.CostEstimate(
            flops=2 * span * steps * depth * (hi - lo),
            bytes_accessed=2 * depth * (hi - lo),
            transcendentals=0,
        ),
        name="output_terms",
    )(order, attended, weights)


def send(values, k, peers):
    return lax.ppermute(values, "tensor", [(t, t ^ k) for t in range(peers)])


def home_device(tokens, norm_gain, w_qkv, w_out, lengths, migrate, page_order, kv_pool, peers):
    slots, steps, width = tokens.shape
    own = lax.axis_index("tensor").astype(jnp.int32)
    order = jnp.bitwise_xor(own, jnp.arange(peers, dtype=jnp.int32))
    by_step = jnp.transpose(tokens, (1, 0, 2))
    floats = by_step.astype(jnp.float32)
    normed = (
        floats * lax.rsqrt(jnp.mean(floats * floats, axis=-1, keepdims=True) + EPS) * norm_gain
    ).astype(jnp.bfloat16)
    projected = None
    for lo, hi in zip(IN_CUTS[:-1], IN_CUTS[1:]):
        part = normed[None, :, :, lo:hi]
        if DIRECT_IN:
            places = [(k,) for k in range(peers)]
            blocks = [part] + [send(part, k, peers) for k in range(1, peers)]
        else:
            places = [tuple(range(0, peers, 2)), tuple(range(1, peers, 2))]
            near = jnp.concatenate([part] + [send(part, k, peers) for k in range(2, peers, 2)])
            blocks = [near, send(near, 1, peers)]
        projected = project(order, blocks, places, w_qkv, lo, hi, projected, hi == width)
    at_home = lax.all_to_all(projected, BOTH, split_axis=0, concat_axis=0, tiled=True)

    slot_ids = jnp.arange(slots, dtype=jnp.int32)
    sorted_lens = jnp.sum(
        jnp.where(migrate[0][:, None] == slot_ids[None, :], lengths[0][:, None], 0), axis=0
    )
    per_head = HEADS // KV_HEADS * steps
    row_step = jnp.arange(per_head, dtype=jnp.int32) % steps
    half = HEAD_DIM // 2
    lanes = jnp.arange(HEAD_DIM, dtype=jnp.int32)
    inverse = ROPE_BASE ** (-((lanes % half).astype(jnp.float32) * 2.0 / HEAD_DIM))
    positions = (sorted_lens[:, None] + row_step[None, :]).astype(jnp.float32)
    angles = positions[..., None] * inverse
    cosine = jnp.cos(angles)
    sine = jnp.where(lanes < half, -1.0, 1.0) * jnp.sin(angles)
    attended = attend(
        lengths,
        migrate,
        page_order,
        at_home,
        cosine,
        sine,
        jnp.broadcast_to(row_step[:, None], (per_head, HEAD_DIM)),
        kv_pool[0],
        peers,
        steps,
    )
    spread = lax.all_to_all(attended, BOTH, split_axis=0, concat_axis=0, tiled=True)
    sums = []
    for lo, hi in zip(OUT_CUTS[:-1], OUT_CUTS[1:]):
        near, far = output_terms(order, spread, w_out, lo, hi, slots, steps)
        paired = near.astype(jnp.float32) + send(far, 1, peers).astype(jnp.float32)
        whole = floats[:, :, lo:hi] + paired[0]
        for k in range(1, peers // 2):
            whole += send(paired[k].astype(jnp.bfloat16), 2 * k, peers).astype(jnp.float32)
        sums.append(whole.astype(jnp.bfloat16))
    return jnp.transpose(jnp.concatenate(sums, axis=2), (1, 0, 2))


def per_device(tokens, norm_gain, w_qkv, w_out, lengths, migrate, page_order, kv_pool, peers, groups):
    arguments = (tokens, norm_gain, w_qkv, w_out, lengths, migrate, page_order, kv_pool)
    if peers == KV_HEADS and groups == tokens.shape[0] and w_qkv.shape[1] % HEAD_DIM == 0:
        return home_device(*arguments, peers)
    return plain_device(*arguments)


def solution(mesh):
    in_specs = (
        P(("group", "tensor"), None, None),
        P(),
        P(None, "tensor"),
        P("tensor", None),
        P(("group", "tensor"), None),
        P(("group", "tensor"), None),
        P(("group", "tensor"), None),
        P(("group", "tensor"), None, None, None, None, None),
    )
    out_specs = P(("group", "tensor"), None, None)
    body = functools.partial(per_device, peers=mesh.shape["tensor"], groups=mesh.shape["group"])
    return jax.shard_map(
        body, mesh=mesh, in_specs=in_specs, out_specs=out_specs, check_vma=False
    )
```

```python
import functools

import jax
import jax.numpy as jnp
from jax import lax
from jax.experimental import pallas as pl
from jax.experimental.pallas import tpu as pltpu
from jax.sharding import PartitionSpec as P

HEADS = 64
KV_HEADS = 8
HEAD_DIM = 128
PAGE = 128
MAX_PAGES = 4


EPS = 1e-05
ROPE_BASE = 500000.0
NEG_FILL = -1e30


def rotate(values, positions):
    half_dim = values.shape[-1] // 2
    inverse = ROPE_BASE ** (-(jnp.arange(half_dim, dtype=jnp.float32) * 2.0 / values.shape[-1]))
    angles = positions.astype(jnp.float32)[..., None] * inverse
    cosine = jnp.cos(angles)[..., None, :]
    sine = jnp.sin(angles)[..., None, :]
    lower_half = values[..., :half_dim]
    upper_half = values[..., half_dim:]
    return jnp.concatenate(
        [lower_half * cosine - upper_half * sine, upper_half * cosine + lower_half * sine], axis=-1
    )


def cache_stats(queries, pages, row_lens):
    row_total, steps_here, head_count, head_dim = queries.shape
    page_count = pages.shape[1]
    kv_heads = pages.shape[3]
    page_len = pages.shape[4]
    grouped = queries.reshape(row_total, steps_here, kv_heads, head_count // kv_heads, head_dim)
    scores = jnp.einsum(
        "rskgd,rbktd->rskgbt", grouped, pages[:, :, 0], preferred_element_type=jnp.float32
    ) * head_dim ** (-0.5)
    places = (
        jnp.arange(page_count, dtype=jnp.int32)[:, None] * page_len
        + jnp.arange(page_len, dtype=jnp.int32)[None, :]
    )
    inside = (places[None] < row_lens[:, None, None])[:, None, None, None]
    page_top = jnp.max(jnp.where(inside, scores, NEG_FILL), axis=-1)
    weights = jnp.where(inside, jnp.exp(scores - page_top[..., None]), 0.0).astype(jnp.bfloat16)
    page_total = jnp.sum(weights.astype(jnp.float32), axis=-1)
    page_acc = jnp.einsum(
        "rskgbt,rbktd->rskgbd", weights, pages[:, :, 1], preferred_element_type=jnp.float32
    )
    top_score = jnp.max(page_top, axis=-1)
    page_scale = jnp.exp(page_top - top_score[..., None])
    return (
        top_score,
        jnp.sum(page_scale * page_total, axis=-1),
        jnp.sum(page_scale[..., None] * page_acc, axis=-2),
    )


def finish(queries, cache_parts, all_keys, all_values):
    row_total, steps_here, head_count, head_dim = queries.shape
    kv_heads = all_keys.shape[2]
    grouped = queries.reshape(row_total, steps_here, kv_heads, head_count // kv_heads, head_dim)
    scores = jnp.einsum(
        "rskgd,rukd->rskgu", grouped, all_keys, preferred_element_type=jnp.float32
    ) * head_dim ** (-0.5)
    allowed = jnp.arange(all_keys.shape[1])[None, :] <= jnp.arange(steps_here)[:, None]
    allowed = allowed[None, :, None, None, :]
    new_top = jnp.max(jnp.where(allowed, scores, NEG_FILL), axis=-1)
    weights = jnp.where(allowed, jnp.exp(scores - new_top[..., None]), 0.0).astype(jnp.bfloat16)
    new_total = jnp.sum(weights.astype(jnp.float32), axis=-1)
    new_acc = jnp.einsum(
        "rskgu,rukd->rskgd", weights, all_values, preferred_element_type=jnp.float32
    )
    cache_top, cache_total, cache_acc = cache_parts
    top_score = jnp.maximum(cache_top, new_top)
    cache_scale = jnp.exp(cache_top - top_score)
    new_scale = jnp.exp(new_top - top_score)
    merged = (cache_scale[..., None] * cache_acc + new_scale[..., None] * new_acc) / (
        cache_scale * cache_total + new_scale * new_total
    )[..., None]
    return merged.reshape(row_total, steps_here, head_count * head_dim).astype(jnp.bfloat16)


def plain_device(tokens, norm_gain, w_qkv, w_out, lengths, migrate, page_order, kv_pool):
    row_lens = lengths[0]
    destinations = migrate[0]
    pool_order = page_order[0]
    page_pool = kv_pool[0]
    row_total = row_lens.shape[0]
    pool_size = page_pool.shape[0]
    slot_ids = jnp.arange(row_total, dtype=jnp.int32)
    sort_keys = destinations * row_total + slot_ids
    row_ranks = jnp.sum((sort_keys[None, :] < sort_keys[:, None]).astype(jnp.int32), axis=1)
    placing = row_ranks[:, None] == slot_ids[None, :]
    pages_used = (row_lens + PAGE - 1) // PAGE
    offsets = jnp.cumsum(pages_used) - pages_used
    sorted_lens = jnp.sum(jnp.where(placing, row_lens[:, None], 0), axis=0)
    sorted_first = jnp.sum(jnp.where(placing, offsets[:, None], 0), axis=0)
    page_slots = jnp.clip(
        sorted_first[:, None] + jnp.arange(MAX_PAGES, dtype=jnp.int32)[None, :], 0, pool_size - 1
    )
    home_pages = page_pool[pool_order[page_slots]]
    new_lens = lax.all_to_all(sorted_lens, "group", split_axis=0, concat_axis=0, tiled=True)
    moved_pages = lax.all_to_all(home_pages, "group", split_axis=0, concat_axis=0, tiled=True)
    width_q = HEADS * HEAD_DIM
    width_k = KV_HEADS * HEAD_DIM
    keys_so_far = jnp.zeros((row_total, 0, KV_HEADS, HEAD_DIM), jnp.bfloat16)
    values_so_far = jnp.zeros((row_total, 0, KV_HEADS, HEAD_DIM), jnp.bfloat16)
    steps_here = tokens.shape[1]
    floats = tokens.astype(jnp.float32)
    normed = (
        floats * lax.rsqrt(jnp.mean(floats * floats, axis=-1, keepdims=True) + EPS) * norm_gain
    ).astype(jnp.bfloat16)
    gathered = jnp.einsum(
        "rsd,dc->rsc",
        lax.all_gather(normed, "tensor", axis=0, tiled=True),
        w_qkv,
        preferred_element_type=jnp.float32,
    ).astype(jnp.bfloat16)
    full_rows = lax.all_to_all(gathered, "tensor", split_axis=0, concat_axis=2, tiled=True)
    positions = new_lens[:, None] + 0 + jnp.arange(steps_here, dtype=jnp.int32)[None, :]
    queries = rotate(
        full_rows[..., :width_q]
        .reshape(row_total, steps_here, HEADS, HEAD_DIM)
        .astype(jnp.float32),
        positions,
    ).astype(jnp.bfloat16)
    keys_here = rotate(
        full_rows[..., width_q : width_q + width_k]
        .reshape(row_total, steps_here, KV_HEADS, HEAD_DIM)
        .astype(jnp.float32),
        positions,
    ).astype(jnp.bfloat16)
    values_here = full_rows[..., width_q + width_k :].reshape(
        row_total, steps_here, KV_HEADS, HEAD_DIM
    )
    all_keys = jnp.concatenate([keys_so_far, keys_here], axis=1)
    all_values = jnp.concatenate([values_so_far, values_here], axis=1)
    attended = finish(queries, cache_stats(queries, moved_pages, new_lens), all_keys, all_values)
    spread = lax.all_to_all(attended, "tensor", split_axis=2, concat_axis=0, tiled=True)
    summed = lax.psum_scatter(
        jnp.einsum("rsc,cd->rsd", spread, w_out, preferred_element_type=jnp.float32).astype(
            jnp.bfloat16
        ),
        "tensor",
        scatter_dimension=0,
        tiled=True,
    ).astype(jnp.float32)
    output = (floats + summed).astype(jnp.bfloat16)
    return output


BOTH = ("tensor", "group")
LOAD_FLOPS = 5 * 10**9
IN_CUTS = (0, 4096, 8192)
OUT_CUTS = (0, 2560, 5632, 8192)
VMEM_LIMIT = 16 * 1024 * 1024
VMEM_WHOLE = pl.BlockSpec(memory_space=pltpu.VMEM)
HBM_WHOLE = pl.BlockSpec(memory_space=pltpu.HBM)


def near_by(array):
    return pltpu.with_memory_space_constraint(array, pltpu.VMEM)


def far_off(array):
    return pltpu.with_memory_space_constraint(array, pltpu.HBM)


def call(body, inputs, specs, out_shape, scratch, flops, moved, name):
    return pl.pallas_call(
        body,
        in_specs=specs,
        out_specs=jax.tree.map(lambda _: VMEM_WHOLE, out_shape),
        out_shape=out_shape,
        scratch_shapes=scratch,
        compiler_params=pltpu.CompilerParams(vmem_limit_bytes=VMEM_LIMIT),
        cost_estimate=pl.CostEstimate(flops=flops, bytes_accessed=moved, transcendentals=0),
        name=name,
    )(*inputs)


def load_kernel(*refs, pieces):
    count = len(pieces)
    sources, targets, sems = refs[:count], refs[count : 2 * count], refs[-1]
    copies = []
    for source, target, parts in zip(sources, targets, pieces):
        size = source.shape[0] // parts
        for part in range(parts):
            rows = pl.ds(part * size, size)
            copies.append(
                pltpu.make_async_copy(source.at[rows], target.at[rows], sems.at[len(copies)])
            )
    for copy in copies:
        copy.start()
    for copy in copies:
        copy.wait()


def load(arrays, pieces, flops):
    return call(
        functools.partial(load_kernel, pieces=pieces),
        [far_off(array) for array in arrays],
        [HBM_WHOLE] * len(arrays),
        [pltpu.VMEM(array.shape, array.dtype) for array in arrays],
        [pltpu.SemaphoreType.DMA((sum(pieces),))],
        flops,
        sum(2 * array.size for array in arrays),
        "load",
    )


def norm_kernel(tokens, gain, *outs):
    values = tokens[...].astype(jnp.float32)
    spread = jnp.mean(values * values, axis=-1, keepdims=True)
    normed = (values * lax.rsqrt(spread + EPS) * gain[...]).astype(jnp.bfloat16)
    lo = 0
    for out in outs:
        out[0] = normed[:, :, lo : lo + out.shape[3]]
        lo += out.shape[3]


def project_kernel(order, *refs, places, tile, lo, last, first):
    blocks = refs[: len(places)]
    weights = refs[len(places)]
    refs = refs[len(places) + 1 :]
    if not first:
        before, refs = refs[0], refs[1:]
    out, lhs, acc = refs[:3]
    peers = order.shape[0]
    _, steps, slots, depth = blocks[0].shape
    span = peers * slots
    for j in range(0, depth, tile):
        for block, ks in zip(blocks, places):
            for n, k in enumerate(ks):
                for s in range(steps):
                    start = s * span + k * slots
                    lhs[start : start + slots, j : j + tile] = block[
                        n, s, :, j : j + tile
                    ].astype(jnp.float32)
        part = jnp.dot(
            lhs[:, j : j + tile].astype(jnp.bfloat16),
            weights[lo + j : lo + j + tile, :],
            preferred_element_type=jnp.float32,
        )
        if j > 0:
            part += acc[...]
        elif not first:
            part += before[...]
        acc[...] = part
    if not last:
        out[...] = acc[...]
        return
    stage = refs[3]
    height = out.shape[1]
    lanes = out.shape[2]
    pieces = acc.shape[1] // lanes
    for c in range(pieces):
        for s in range(steps):
            stage[pl.ds(c * steps + s, span, stride=height), :] = acc[
                s * span : (s + 1) * span, c * lanes : (c + 1) * lanes
            ]
    for extra in range(pieces * steps, height):
        stage[pl.ds(extra, span, stride=height), :] = jnp.zeros((span, lanes), jnp.float32)
    for k in range(peers):
        for i in range(slots):
            place = (k * slots + i) * height
            out[order[k] * slots + i] = stage[place : place + height, :].astype(jnp.bfloat16)


def project(order, blocks, places, weights, lo, hi, before, last):
    peers = order.shape[0]
    _, steps, slots, depth = blocks[0].shape
    width = weights.shape[1]
    tile = 1024
    rows = peers * steps * slots
    height = -(-(width // HEAD_DIM * steps) // 16) * 16
    first = before is None
    operands = [near_by(array) for array in list(blocks) + [weights]]
    if not first:
        operands.append(near_by(before))
    scratch = [pltpu.VMEM((rows, depth), jnp.float32), pltpu.VMEM((rows, width), jnp.float32)]
    if last:
        out_shape = pltpu.VMEM((peers * slots, height, HEAD_DIM), jnp.bfloat16)
        scratch.append(pltpu.VMEM((peers * slots * height, HEAD_DIM), jnp.float32))
    else:
        out_shape = pltpu.VMEM((rows, width), jnp.float32)
    return call(
        functools.partial(
            project_kernel, places=places, tile=tile, lo=lo, last=last, first=first
        ),
        [order] + operands,
        [pl.BlockSpec(memory_space=pltpu.SMEM)] + [VMEM_WHOLE] * len(operands),
        out_shape,
        scratch,
        2 * rows * width * (hi - lo),
        2 * width * (hi - lo),
        "project",
    )


def attend_kernel(
    lens, dest, order, qkv, cosine, sine, row_step, pool, out,
    pages, rows_f, fresh, queries, sems, *, peers, steps,
):
    slots = cosine.shape[0]
    per_head = cosine.shape[1]
    kv_heads, page_len, dim = pages.shape[2:]
    per_peer = rows_f.shape[1] // peers
    scale = dim ** (-0.5)
    used = [(lens[0, j] + page_len - 1) // page_len for j in range(slots)]
    starts = [jnp.int32(0)]
    for j in range(slots - 1):
        starts.append(starts[-1] + used[j])

    def pick(values, i):
        found = jnp.int32(0)
        for j in range(slots):
            found = jnp.where(dest[0, j] == i, values[j], found)
        return found

    row_used = [pick(used, i) for i in range(slots)]
    row_start = [pick(starts, i) for i in range(slots)]
    row_len = [pick([lens[0, j] for j in range(slots)], i) for i in range(slots)]

    def fetch(slot, source):
        return pltpu.make_async_copy(pool.at[source], pages.at[slot], sems.at[slot])

    for i in range(slots):
        for b in range(MAX_PAGES):

            @pl.when(b < row_used[i])
            def _(i=i, b=b):
                fetch(i * MAX_PAGES + b, order[0, row_start[i] + b]).start()

    lane = lax.broadcasted_iota(jnp.int32, (per_head, page_len), 1)
    steps_of = row_step[...]
    edge = kv_heads * per_head
    span = kv_heads * steps
    fresh[...] = jnp.zeros(fresh.shape, fresh.dtype)

    def turn(values, i):
        return values * cosine[i] + pltpu.roll(values, dim // 2, 1) * sine[i]

    for i in range(slots):
        for peer in range(peers):
            rows_f[i, peer * per_peer : (peer + 1) * per_peer, :] = qkv[
                peer * slots + i, 0:per_peer, :
            ].astype(jnp.float32)
        for h in range(kv_heads):
            queries[i, h] = turn(
                rows_f[i, h * per_head : (h + 1) * per_head, :], i
            ).astype(jnp.bfloat16)
        fresh[i, 0, 0:span, :] = turn(rows_f[i, edge : edge + span, :], i).astype(jnp.bfloat16)
        fresh[i, 1, 0:span, :] = rows_f[i, edge + span : edge + 2 * span, :].astype(jnp.bfloat16)

    together = 4
    tail_lane = lax.broadcasted_iota(jnp.int32, (per_head, fresh.shape[2]), 1)
    tail_steps = row_step[:, 0 : fresh.shape[2]]

    def attend_row(i, count):
        for b in range(count):
            fetch(i * MAX_PAGES + b, 0).wait()
        live = [lane + b * page_len < row_len[i] for b in range(count)]
        for base in range(0, kv_heads, together):
            group = range(base, base + together)

            def score(h, keys, inside):
                found = lax.dot_general(
                    queries[i, h], keys, (((1,), (1,)), ((), ())),
                    preferred_element_type=jnp.float32,
                )
                return jnp.where(inside, found * scale, NEG_FILL)

            scores = [
                [score(h, pages[i * MAX_PAGES + b, 0, h], live[b]) for b in range(count)]
                for h in group
            ]
            tails = [
                score(
                    h,
                    fresh[i, 0],
                    (tail_lane >= h * steps) & (tail_lane <= h * steps + tail_steps),
                )
                for h in group
            ]
            tops = [
                jnp.maximum(
                    jnp.max(functools.reduce(jnp.maximum, row), axis=1, keepdims=True),
                    jnp.max(tail, axis=1, keepdims=True),
                )
                for row, tail in zip(scores, tails)
            ]
            weights = [
                [jnp.exp(block - high).astype(jnp.bfloat16) for block in row]
                for row, high in zip(scores, tops)
            ]
            ends = [jnp.exp(tail - high).astype(jnp.bfloat16) for tail, high in zip(tails, tops)]
            sums = [
                jnp.sum(
                    functools.reduce(jnp.add, [w.astype(jnp.float32) for w in row]),
                    axis=1,
                    keepdims=True,
                )
                + jnp.sum(end.astype(jnp.float32), axis=1, keepdims=True)
                for row, end in zip(weights, ends)
            ]
            for h, row, end, mass in zip(group, weights, ends, sums):
                total = jnp.dot(end, fresh[i, 1], preferred_element_type=jnp.float32)
                for b in range(count):
                    total += jnp.dot(
                        row[b],
                        pages[i * MAX_PAGES + b, 1, h],
                        preferred_element_type=jnp.float32,
                    )
                out[h * slots + i] = (total / mass).astype(jnp.bfloat16)

    for i in range(slots):
        for count in range(1, MAX_PAGES + 1):
            pl.when(row_used[i] == count)(functools.partial(attend_row, i, count))


def attend(lengths, migrate, page_order, qkv, cosine, sine, row_step, pool, peers, steps):
    slots, per_head, dim = cosine.shape
    _, _, kv_heads, page_len, _ = pool.shape
    smem = pl.BlockSpec(memory_space=pltpu.SMEM)
    per_peer = (kv_heads * per_head + 2 * kv_heads * steps) // peers
    work = slots * kv_heads * per_head * dim * page_len * MAX_PAGES
    arrays = [near_by(array) for array in (qkv, cosine, sine, row_step)]
    return call(
        functools.partial(attend_kernel, peers=peers, steps=steps),
        [lengths, migrate, page_order] + arrays + [far_off(pool)],
        [smem] * 3 + [VMEM_WHOLE] * 4 + [HBM_WHOLE],
        pltpu.VMEM((kv_heads * slots, per_head, dim), jnp.bfloat16),
        [
            pltpu.VMEM((slots * MAX_PAGES,) + pool.shape[1:], pool.dtype),
            pltpu.VMEM((slots, peers * per_peer, dim), jnp.float32),
            pltpu.VMEM((slots, 2, -(-(kv_heads * steps) // 16) * 16, dim), jnp.bfloat16),
            pltpu.VMEM((slots, kv_heads, per_head, dim), jnp.bfloat16),
            pltpu.SemaphoreType.DMA((slots * MAX_PAGES,)),
        ],
        4 * work,
        2 * pool.size,
        "attend",
    )


def output_kernel(order, attended, weights, near, far, wide, lhs, tiles, sems, *, steps, lo):
    peers = order.shape[0]
    span, height, lanes = attended.shape
    slots = span // peers
    count, _, tile = tiles.shape

    def fetch(j):
        return pltpu.make_async_copy(
            weights.at[:, pl.ds(lo + j * tile, tile)], tiles.at[j], sems.at[j]
        )

    for j in range(count):
        fetch(j).start()
    for k in range(peers):
        for i in range(slots):
            place = (k * slots + i) * height
            wide[place : place + height, :] = attended[order[k] * slots + i].astype(jnp.float32)
    for c in range(height // steps):
        for s in range(steps):
            lhs[s * span : (s + 1) * span, c * lanes : (c + 1) * lanes] = wide[
                pl.ds(c * steps + s, span, stride=height), :
            ].astype(jnp.bfloat16)
    for j in range(count):
        fetch(j).wait()
        term = jnp.dot(lhs[...], tiles[j], preferred_element_type=jnp.float32)
        for k in range(peers):
            for s in range(steps):
                start = s * span + k * slots
                outs = far if k % 2 else near
                outs[k // 2, s, :, j * tile : (j + 1) * tile] = term[
                    start : start + slots, :
                ].astype(jnp.bfloat16)


def output_terms(order, attended, weights, lo, hi, slots, steps):
    span, height, lanes = attended.shape
    depth = weights.shape[0]
    tile = 512
    shape = pltpu.VMEM((span // slots // 2, steps, slots, hi - lo), jnp.bfloat16)
    return call(
        functools.partial(output_kernel, steps=steps, lo=lo),
        [order, near_by(attended), far_off(weights)],
        [pl.BlockSpec(memory_space=pltpu.SMEM), VMEM_WHOLE, HBM_WHOLE],
        [shape, shape],
        [
            pltpu.VMEM((span * height, lanes), jnp.float32),
            pltpu.VMEM((span * steps, depth), jnp.bfloat16),
            pltpu.VMEM(((hi - lo) // tile, depth, tile), jnp.bfloat16),
            pltpu.SemaphoreType.DMA(((hi - lo) // tile,)),
        ],
        2 * span * steps * depth * (hi - lo),
        2 * depth * (hi - lo),
        "output_terms",
    )


def send(values, k, peers):
    return lax.ppermute(values, "tensor", [(t, t ^ k) for t in range(peers)])


def pair_kernel(near, arrived, own, *outs):
    own[...] = near[0].astype(jnp.float32) + arrived[0].astype(jnp.float32)
    for k, out in enumerate(outs, 1):
        out[...] = (near[k].astype(jnp.float32) + arrived[k].astype(jnp.float32)).astype(
            jnp.bfloat16
        )


def pair(near, arrived):
    shape = near.shape[1:]
    return call(
        pair_kernel,
        [near_by(near), near_by(arrived)],
        [VMEM_WHOLE] * 2,
        [pltpu.VMEM(shape, jnp.float32)]
        + [pltpu.VMEM(shape, jnp.bfloat16)] * (near.shape[0] - 1),
        [],
        near.size,
        0,
        "pair",
    )


def home_device(tokens, norm_gain, w_qkv, w_out, lengths, migrate, page_order, kv_pool, peers):
    slots, steps, width = tokens.shape
    own = lax.axis_index("tensor").astype(jnp.int32)
    order = jnp.bitwise_xor(own, jnp.arange(peers, dtype=jnp.int32))
    by_step = jnp.transpose(tokens, (1, 0, 2))
    parts = call(
        norm_kernel,
        [by_step, norm_gain[None, None, :]],
        [VMEM_WHOLE] * 2,
        [
            pltpu.VMEM((1, steps, slots, hi - lo), jnp.bfloat16)
            for lo, hi in zip(IN_CUTS[:-1], IN_CUTS[1:])
        ],
        [],
        8 * tokens.size,
        2 * tokens.size,
        "norm",
    )
    (qkv_here,) = load([w_qkv], [16], LOAD_FLOPS)
    projected = None
    places = [tuple(range(0, peers, 2)), tuple(range(1, peers, 2))]
    for part, lo, hi in zip(parts, IN_CUTS[:-1], IN_CUTS[1:]):
        near = jnp.concatenate([part] + [send(part, k, peers) for k in range(2, peers, 2)])
        blocks = [near, send(near, 1, peers)]
        projected = project(order, blocks, places, qkv_here, lo, hi, projected, hi == width)
    at_home = lax.all_to_all(projected, BOTH, split_axis=0, concat_axis=0, tiled=True)

    slot_ids = jnp.arange(slots, dtype=jnp.int32)
    sorted_lens = jnp.sum(
        jnp.where(migrate[0][:, None] == slot_ids[None, :], lengths[0][:, None], 0), axis=0
    )
    per_head = HEADS // KV_HEADS * steps
    row_step = jnp.arange(per_head, dtype=jnp.int32) % steps
    half = HEAD_DIM // 2
    lanes = jnp.arange(HEAD_DIM, dtype=jnp.int32)
    inverse = ROPE_BASE ** (-((lanes % half).astype(jnp.float32) * 2.0 / HEAD_DIM))
    positions = (sorted_lens[:, None] + row_step[None, :]).astype(jnp.float32)
    angles = positions[..., None] * inverse
    cosine = jnp.cos(angles)
    sine = jnp.where(lanes < half, -1.0, 1.0) * jnp.sin(angles)
    attended = attend(
        lengths,
        migrate,
        page_order,
        at_home,
        cosine,
        sine,
        jnp.broadcast_to(row_step[:, None], (per_head, HEAD_DIM)),
        kv_pool[0],
        peers,
        steps,
    )
    spread = lax.all_to_all(attended, BOTH, split_axis=0, concat_axis=0, tiled=True)
    sums = []
    for lo, hi in zip(OUT_CUTS[:-1], OUT_CUTS[1:]):
        near, far = output_terms(order, spread, w_out, lo, hi, slots, steps)
        own, *others = pair(near, send(far, 1, peers))
        whole = by_step[:, :, lo:hi].astype(jnp.float32) + own
        for k, other in enumerate(others, 1):
            whole += send(other, 2 * k, peers).astype(jnp.float32)
        sums.append(whole.astype(jnp.bfloat16))
    return jnp.transpose(jnp.concatenate(sums, axis=2), (1, 0, 2))


def per_device(tokens, norm_gain, w_qkv, w_out, lengths, migrate, page_order, kv_pool, peers, groups):
    arguments = (tokens, norm_gain, w_qkv, w_out, lengths, migrate, page_order, kv_pool)
    if peers == KV_HEADS and groups == tokens.shape[0] and w_qkv.shape[1] % HEAD_DIM == 0:
        return home_device(*arguments, peers)
    return plain_device(*arguments)


def solution(mesh):
    in_specs = (
        P(("group", "tensor"), None, None),
        P(),
        P(None, "tensor"),
        P("tensor", None),
        P(("group", "tensor"), None),
        P(("group", "tensor"), None),
        P(("group", "tensor"), None),
        P(("group", "tensor"), None, None, None, None, None),
    )
    out_specs = P(("group", "tensor"), None, None)
    body = functools.partial(per_device, peers=mesh.shape["tensor"], groups=mesh.shape["group"])
    return jax.shard_map(
        body, mesh=mesh, in_specs=in_specs, out_specs=out_specs, check_vma=False
    )
```
